32 devices in a mesh: gz: 16 (over z, x, core), xy: 2 (over y).
Axes of the slice: x: 2, y: 2, z: 4, core: 2. Of those that a mesh axis runs over, the one named last changes fastest.
Arguments:
- coords: float32 [3, 32, 4, 128], P(None, 'gz', 'xy'), may hold values from 0 to 1
- species: int32 [32, 4, 128], P('gz', 'xy'), may hold values from 0 to 7
- centers: int32 [32, 4, 128], P('gz', 'xy'), may hold values from 0 to 127
- others: int32 [32, 4, 128], P('gz', 'xy'), may hold values from 0 to 1151
- live_count: int32 [32, 4], P('gz', 'xy'), may hold values from 42 to 128
- in_weight: float32 [24, 128], replicated, may hold values from -1.25 to 1.25
- env_weight: float32 [128, 32], replicated, may hold values from -0.5 to 0.5
- up_weight: float32 [160, 128], replicated, may hold values from -0.5 to 0.5
- out_weight: float32 [128], replicated, may hold values from -0.5 to 0.5
Outputs:
- atom_energy: float32 [32, 4, 128], P('gz', 'xy')
- forces: float32 [3, 32, 4, 128], P(None, 'gz', 'xy')
The draws below stay inside these ranges and needn't reach their ends.
Inputs may be any that keep to these rules, and one draw needn't show every extreme that they name: Edge slots at or after live_count of a bin are padding; at most 128 are live.
All inputs are finite; a program needn't handle non-finite values.
Results may differ from the reference program's by a relative error of at most 0.0018.
Values may be sent and summed in bfloat16 or wider, within the bound.
A program may use at most 64 MiB of HBM per device.

```python
import jax
import jax.numpy as jnp
from jax import lax

BIN = 128
NB = 8
SPEC = 8
LAT = 128
CH = 32
EDGES = 128
NBZ = 32
NBX = 4


def touch_ends(array, own_key, least, largest):
    longest = array.shape.index(max(array.shape))
    spots = []
    for shift in (0, 1):
        where = [jax.random.randint(jax.random.fold_in(own_key, axis), (), 0, length) for axis, length in enumerate(array.shape)]
        where[longest] = (where[longest] + shift) % array.shape[longest]
        spots.append(tuple(where))
    return array.at[spots[0]].set(least).at[spots[1]].set(largest)


def levels(rng, shape, cuts, smallest, high):
    gain, own = 1.0, jax.random.fold_in(rng, 6)
    for axis_at, shards_of in cuts:
        steps = jnp.exp(jax.random.uniform(jax.random.fold_in(own, axis_at), (shards_of,), jnp.float32, smallest / len(cuts), high / len(cuts)))
        gain = gain * jnp.repeat(steps, shape[axis_at] // shards_of).reshape([-1 if axis == axis_at else 1 for axis in range(len(shape))])
    return gain


def scatter_about(key, extent, spread, reach, kind=jnp.bfloat16):
    return jnp.clip(spread * jax.random.normal(key, extent, jnp.float32), -reach, reach).astype(kind)


def setup_inputs(seed: int = 0) -> dict:
    arg_keys = jax.random.split(jax.random.key(seed), 10)
    return {
        "coords": jnp.clip(1.0 * jax.random.uniform(arg_keys[0], (3, NBZ, NBX, BIN), jnp.float32) ** levels(arg_keys[0], (3, NBZ, NBX, BIN), ((1, 16), (2, 2)), -0.2, 0.2), 0.0, 1.0),
        "species": touch_ends(jax.random.randint(arg_keys[1], (NBZ, NBX, BIN), 0, SPEC), jax.random.fold_in(arg_keys[1], 1), 0, SPEC - 1).astype(jnp.int32),
        "centers": touch_ends(jax.random.randint(arg_keys[2], (NBZ, NBX, EDGES), 0, BIN), jax.random.fold_in(arg_keys[2], 1), 0, BIN - 1).astype(jnp.int32),
        "others": touch_ends(jax.random.randint(arg_keys[3], (NBZ, NBX, EDGES), 0, 9 * BIN), jax.random.fold_in(arg_keys[3], 1), 0, (9 * BIN) - 1).astype(jnp.int32),
        "live_count": touch_ends(jax.random.randint(arg_keys[4], (NBZ, NBX), EDGES // 3, EDGES + 1), jax.random.fold_in(arg_keys[4], 1), EDGES // 3, EDGES).astype(jnp.int32),
        "in_weight": scatter_about(arg_keys[5], (NB + 2 * SPEC, LAT), (NB + 2 * SPEC) ** -0.5, 1.25, jnp.float32),
        "env_weight": scatter_about(arg_keys[6], (LAT, CH), LAT ** -0.5, 0.5, jnp.float32),
        "up_weight": scatter_about(arg_keys[7], (LAT + CH, LAT), (LAT + CH) ** -0.5, 0.5, jnp.float32),
        "out_weight": scatter_about(arg_keys[8], (LAT,), LAT ** -0.5, 0.5, jnp.float32),
    }


SOFTEN = 0.01
CUTOFF = 3.5
HIGH = lax.Precision.HIGHEST

def neighbourhood(lattice):
    depth_bins = lattice.shape[-3] - 2
    span_bins = lattice.shape[-2] - 2
    blocks = []
    for offset in range(9):
        start_z = offset // 3
        start_x = offset % 3
        blocks.append(lattice[..., start_z:start_z + depth_bins, start_x:start_x + span_bins, :])
    return jnp.concatenate(blocks, axis=-1)

def pick(lattice, indices):
    return jnp.take_along_axis(lattice, jnp.broadcast_to(indices, lattice.shape[:1] + indices.shape), axis=-1)

def live_mask(live_count, edge_count):
    return (jnp.arange(edge_count)[None, None, :] < live_count[..., None]).astype(jnp.float32)

def geometry(coord_ext, spec_ext, centers, others, in_weight):
    interior = coord_ext[:, 1:-1, 1:-1]
    at_center = pick(interior, centers)
    at_other = pick(neighbourhood(coord_ext), others)
    placement = others // 128
    shift_z = (placement // 3 - 1).astype(jnp.float32)
    shift_x = (placement % 3 - 1).astype(jnp.float32)
    along_z = shift_z + at_other[0] - at_center[0]
    across = shift_x + at_other[1] - at_center[1]
    along_y = at_other[2] - at_center[2]
    distance = jnp.sqrt(along_z * along_z + across * across + along_y * along_y + SOFTEN)
    scaled = distance / CUTOFF
    envelope = (1.0 - scaled * scaled) ** 2
    orders = jnp.arange(1, NB + 1).astype(jnp.float32)[:, None, None, None]
    radial = jnp.sin(orders * jnp.pi * scaled[None]) / distance[None] * envelope[None]
    species_ids = jnp.arange(SPEC).astype(spec_ext.dtype)[:, None, None, None]
    spec_center = pick(spec_ext[None, 1:-1, 1:-1], centers)
    spec_other = pick(neighbourhood(spec_ext[None]), others)
    inputs = jnp.concatenate([radial, (spec_center == species_ids).astype(jnp.float32), (spec_other == species_ids).astype(jnp.float32)], axis=0)
    latent = jax.nn.silu(jnp.einsum('kabe,kl->labe', inputs, in_weight, precision=HIGH))
    harmonics = jnp.stack([jnp.ones_like(distance), along_z / distance, across / distance, along_y / distance])
    return (latent, harmonics, envelope)

def features(latent, harmonics, centers, live_count, env_weight):
    edge_count = centers.shape[-1]
    weights = jnp.einsum('labe,lc->cabe', latent, env_weight, precision=HIGH) * live_mask(live_count, edge_count)[None]
    messages = (weights[:, None] * harmonics[None]).reshape((-1,) + centers.shape)
    one_hot = (centers[..., None] == jnp.arange(128)).astype(jnp.float32)
    return jnp.einsum('fabe,aben->fabn', messages, one_hot, precision=HIGH) * (128.0 / edge_count)

def energy(latent, envelope, feature_ext, centers, others, live_count, up_weight, out_weight):
    channels = feature_ext.shape[0] // 4
    feat_center = pick(feature_ext[:, 1:-1, 1:-1], centers)
    feat_other = pick(neighbourhood(feature_ext), others)
    products = (feat_center * feat_other).reshape((channels, 4) + centers.shape).sum(axis=1)
    joined = jnp.concatenate([latent, products], axis=0)
    hidden = jax.nn.silu(jnp.einsum('kabe,kl->labe', joined, up_weight, precision=HIGH))
    edge_energy = jnp.einsum('labe,l->abe', hidden, out_weight, precision=HIGH) * envelope * live_mask(live_count, centers.shape[-1])
    one_hot = (centers[..., None] == jnp.arange(128)).astype(jnp.float32)
    atom_energy = jnp.einsum('abe,aben->abn', edge_energy, one_hot, precision=HIGH)
    return (jnp.sum(edge_energy), atom_energy)

def wrap_pad(lattice, first_dim):
    widths = [(0, 0)] * lattice.ndim
    widths[first_dim] = (1, 1)
    widths[first_dim + 1] = (1, 1)
    return jnp.pad(lattice, widths, mode='wrap')

def reference(coords, species, centers, others, live_count, in_weight, env_weight, up_weight, out_weight):
    row_count = coords.shape[1]
    spec_pad = wrap_pad(species, 0)
    row_ids = jnp.arange(row_count).astype(jnp.int32)

    def total(coords_now):
        coord_pad = wrap_pad(coords_now, 1)

        def row_latent(row_index):
            coord_block = lax.dynamic_slice_in_dim(coord_pad, row_index, 3, 1)
            spec_block = lax.dynamic_slice_in_dim(spec_pad, row_index, 3, 0)
            center_row = lax.dynamic_slice_in_dim(centers, row_index, 1, 0)
            other_row = lax.dynamic_slice_in_dim(others, row_index, 1, 0)
            live_row = lax.dynamic_slice_in_dim(live_count, row_index, 1, 0)
            return (geometry(coord_block, spec_block, center_row, other_row, in_weight), center_row, other_row, live_row)

        def feature_row(row_index):
            (latent, harmonics, envelope), center_row, other_row, live_row = row_latent(row_index)
            return features(latent, harmonics, center_row, live_row, env_weight)
        stacked = lax.map(jax.checkpoint(feature_row), row_ids)
        features_all = jnp.moveaxis(stacked[:, :, 0], 0, 1)
        rounded = lax.optimization_barrier(features_all.astype(jnp.bfloat16)).astype(jnp.float32)
        through = features_all + lax.stop_gradient(rounded - features_all)
        feature_pad = wrap_pad(through, 1)

        def energy_row(row_index):
            (latent, harmonics, envelope), center_row, other_row, live_row = row_latent(row_index)
            feature_block = lax.dynamic_slice_in_dim(feature_pad, row_index, 3, 1)
            return energy(latent, envelope, feature_block, center_row, other_row, live_row, up_weight, out_weight)
        row_sums, row_atoms = lax.map(jax.checkpoint(energy_row), row_ids)
        return (jnp.sum(row_sums), row_atoms[:, 0])
    (energy_total, atom_energy), gradient = jax.value_and_grad(total, has_aux=True)(coords)
    return (atom_energy, -gradient)
```

```python
import functools
import math

import jax
import jax.numpy as jnp
from jax import lax
from jax.experimental import pallas as pl
from jax.experimental.pallas import tpu as pltpu
from jax.sharding import PartitionSpec as P

SOFTEN = 0.01
CUTOFF = 3.5
F32 = jnp.float32
BF16 = jnp.bfloat16
MESH = pl.DeviceIdType.MESH


def rounded(x):
    return x.astype(BF16).astype(F32)


def split(x):
    high = x.astype(BF16)
    return high, (x - high.astype(F32)).astype(BF16)


def dot(a, b):
    return jnp.dot(a, b, preferred_element_type=F32)


def dot_t(a, b):
    return lax.dot_general(a, b, (((1,), (1,)), ((), ())), preferred_element_type=F32)


def join(parts, axis):
    return parts[0] if len(parts) == 1 else jnp.concatenate(parts, axis=axis)


def neighbours(nz, nx):
    slots = {(0, 0): 0}
    for dz in (-1, 0, 1):
        for dx in (-1, 0, 1):
            slots.setdefault((dz % nz, dx % nx), len(slots))
    return slots


def kernel(
    nz, nx, bz, bx, nb, spec, ch, lat,
    coords_ref, species_ref, centers_ref, others_ref, live_ref, in_ref, env_ref, up_ref, out_ref,
    energy_ref, forces_ref,
    own, halo, tab, ct, ot, rows_live, rows_p, geo, xs, sins, coss, rad, harm,
    l2, dsilu, wts, feat, dfeat, dlat_own, env_grad, dharm, drad, gr, grad, back,
    send1, recv1, send2, recv2,
):
    n = coords_ref.shape[-1]
    slots = neighbours(nz, nx)
    me_z, me_x = lax.axis_index("gz"), lax.axis_index("xy")
    others_list = [(key, s) for key, s in slots.items() if s > 0]

    def device(key):
        return (lax.rem(me_z + key[0], nz), lax.rem(me_x + key[1], nx))

    def mirror(key):
        return slots[((-key[0]) % nz, (-key[1]) % nx)]

    barrier = pltpu.get_barrier_semaphore()
    for key, _ in others_list:
        pl.semaphore_signal(barrier, inc=1, device_id=device(key), device_id_type=MESH)

    lane = lax.broadcasted_iota(jnp.int32, (1, n), 1)
    for a in range(bz):
        for b in range(bx):
            alive = (lane < live_ref[a, b]).astype(F32)
            own[a, b] = jnp.concatenate(
                [
                    coords_ref[:, a, b, :],
                    species_ref[a, b : b + 1, :].astype(F32),
                    centers_ref[a, b : b + 1, :].astype(F32),
                    others_ref[a, b : b + 1, :].astype(F32),
                    alive,
                    jnp.zeros((1, n), F32),
                ],
                axis=0,
            )
    pl.semaphore_wait(barrier, len(others_list))
    first = []
    for key, s in others_list:
        t = mirror(key)
        copy = pltpu.make_async_remote_copy(
            src_ref=own, dst_ref=halo.at[t - 1], send_sem=send1.at[s - 1],
            recv_sem=recv1.at[t - 1], device_id=device(key), device_id_type=MESH,
        )
        copy.start()
        first.append(copy)

    w_in = in_ref[...]
    w_hi = rounded(w_in)
    w_lo = w_in - w_hi
    w_rows = jnp.concatenate(
        [w_hi[:nb], w_lo[:nb], w_hi[:nb], w_hi[nb:], w_lo[nb:],
         jnp.zeros((lat - 3 * nb - 4 * spec, lat), F32)], axis=0)
    kin = (3 * nb + 4 * spec + 15) // 16 * 16
    in_t = w_rows.T.astype(BF16)[:, :kin]
    pad8 = jnp.zeros((nb, lat), F32)
    wr_hi = jnp.concatenate([w_hi[:nb], pad8], axis=0).astype(BF16)
    wr_lo = jnp.concatenate([w_lo[:nb], pad8], axis=0).astype(BF16)
    wr3 = jnp.concatenate([wr_hi, wr_hi, wr_lo], axis=1)
    env_t = env_ref[...].T
    et_hi = rounded(env_t)
    et_lo = env_t - et_hi
    env_t3 = jnp.concatenate([et_hi, et_hi, et_lo], axis=1).astype(BF16)
    kpad = -(3 * ch) % lat
    env3 = jnp.concatenate(
        [et_hi, et_hi, et_lo] + ([jnp.zeros((kpad, lat), F32)] if kpad else []), axis=0
    ).T.astype(BF16)
    up = up_ref[...]
    up_hi = rounded(up)
    up_lo = up - up_hi
    up3 = jnp.concatenate([up_hi, up_hi, up_lo], axis=1).astype(BF16)
    up_t = jnp.concatenate(
        [x.T.astype(BF16) for x in (up_hi[:lat], up_hi[:lat], up_lo[:lat])]
        + [jnp.concatenate(
            [up_hi[lat:], up_hi[lat:], up_lo[lat:]]
            + ([jnp.zeros((kpad, lat), F32)] if kpad else []), axis=0).T.astype(BF16)],
        axis=1)
    out_col = jnp.broadcast_to(out_ref[...], (n, lat)).T

    for copy in first:
        copy.wait()

    def place(a, b):
        return slots[((a // bz - 1) % nz, (b // bx - 1) % nx)], a % bz, b % bx

    def block(a, b):
        s, i, j = place(a, b)
        return own[i, j] if s == 0 else halo[s - 1, i, j]

    window_z = range(bz - 2, 2 * bz + 2)
    window_x = range(bx - 2, 2 * bx + 2)
    for a in window_z:
        for b in window_x:
            part = block(a, b)
            hi = rounded(part)
            tab[a, b] = jnp.concatenate([hi, part - hi], axis=0).astype(BF16)

    cells = [(a, b) for a in range(bz - 1, 2 * bz + 1) for b in range(bx - 1, 2 * bx + 1)]
    cx = bx + 2
    total = len(cells)
    row_n = lax.broadcasted_iota(jnp.int32, (n, n), 0)
    row_s = lax.broadcasted_iota(jnp.int32, (spec, n), 0).astype(F32)
    for i, (a, b) in enumerate(cells):
        part = block(a, b)
        c = part[4:5].astype(jnp.int32)
        o = part[5:6].astype(jnp.int32)
        p = o >> 7
        hot_c = (row_n == c).astype(F32).astype(BF16)
        hot_o = (row_n == (o & 127)).astype(F32).astype(BF16)
        ct[i] = hot_c
        ot[i] = hot_o
        at_c = dot(tab[a, b], hot_c)
        at_c = at_c[:8] + at_c[8:]
        around = jnp.concatenate(
            [tab[a + dz, b + dx] for dz in (-1, 0, 1) for dx in (-1, 0, 1)], axis=0)
        got = dot(around, hot_o)
        at_o = jnp.zeros((8, n), F32)
        for off in range(9):
            at_o = jnp.where(p == off, got[16 * off : 16 * off + 8] + got[16 * off + 8 : 16 * off + 16], at_o)
        diff = at_o - at_c
        up3_ = (p >= 3).astype(jnp.int32) + (p >= 6).astype(jnp.int32)
        geo[0, i : i + 1] = diff[0:1] + (up3_ - 1).astype(F32)
        geo[1, i : i + 1] = diff[1:2] + (p - 3 * up3_ - 1).astype(F32)
        geo[2, i : i + 1] = diff[2:3]
        xs[:spec, i * n : (i + 1) * n] = (row_s == at_c[3:4]).astype(F32)
        xs[spec:, i * n : (i + 1) * n] = (row_s == at_o[3:4]).astype(F32)
        rows_live[i : i + 1] = part[6:7]
        rows_p[i : i + 1] = p

    r = [geo[m] for m in range(3)]
    dist = jnp.sqrt(r[0] * r[0] + r[1] * r[1] + r[2] * r[2] + SOFTEN)
    inv = 1.0 / dist
    q = dist / CUTOFF
    rest = 1.0 - q * q
    envelope = rest * rest
    scale = inv * envelope
    s1 = jnp.sin(math.pi * q)
    c1 = jnp.cos(math.pi * q)
    s0, c0, sk, ck = jnp.zeros_like(s1), jnp.ones_like(c1), s1, c1
    for k in range(nb):
        sins[k] = sk
        coss[k] = ck
        rad[k] = sk * scale
        s0, sk = sk, 2.0 * c1 * sk - s0
        c0, ck = ck, 2.0 * c1 * ck - c0
    for m in range(3):
        harm[m] = r[m] * inv
    env_grad[...] = jnp.zeros_like(env_grad)
    geo[3] = envelope

    interior = {}
    for i, (a, b) in enumerate(cells):
        if bz <= a < 2 * bz and bx <= b < 2 * bx:
            interior[i] = (a - bz) * bx + (b - bx)

    group = 2 if total % 2 == 0 else 1
    for g in range(0, total, group):
        ids = list(range(g, g + group))
        span = slice(g * n, (g + group) * n)
        radial = join([rad[:, i, :] for i in ids], 1)
        rh = rounded(radial)
        x_s = xs[:, span]
        parts = [rh, rh, radial - rh, x_s, x_s]
        fill = kin - 3 * nb - 4 * spec
        if fill:
            parts.append(jnp.zeros((fill, group * n), F32))
        pre = dot(in_t, jnp.concatenate(parts, axis=0).astype(BF16))
        sig = 1.0 / (1.0 + jnp.exp(-pre))
        latent = pre * sig
        dsilu[:, span] = sig + latent * (1.0 - sig)
        lh, ll = split(latent)
        for t, i in enumerate(ids):
            if i in interior:
                l2[interior[i], 0] = lh[:, t * n : (t + 1) * n]
                l2[interior[i], 1] = ll[:, t * n : (t + 1) * n]
        alive = join([rows_live[i : i + 1] for i in ids], 1)
        w = dot(env_t3, jnp.concatenate([lh, ll, lh], axis=0)) * alive
        wts[:, span] = w
        msgs = jnp.concatenate(
            [w] + [w * join([harm[m, i : i + 1] for i in ids], 1) for m in range(3)], axis=0)
        mh, ml = split(msgs)
        for t, i in enumerate(ids):
            cut = slice(t * n, (t + 1) * n)
            hot_c = ct[i]
            feat[:, i * n : (i + 1) * n] = dot_t(
                jnp.concatenate([mh[:, cut], ml[:, cut]], axis=1),
                jnp.concatenate([hot_c, hot_c], axis=1)).astype(BF16)

    dfeat[...] = jnp.zeros_like(dfeat)
    row_8 = lax.broadcasted_iota(jnp.int32, (16, n), 0)
    for i, k in interior.items():
        hot_c, hot_o = ct[i], ot[i]
        p = rows_p[i : i + 1]
        env_row = geo[3, i : i + 1]
        alive = rows_live[i : i + 1]
        f_c = dot(feat[:, i * n : (i + 1) * n], hot_c)
        f_o = None
        hots = []
        for dz in range(3):
            start = i + (dz - 1) * cx - 1
            hot3 = jnp.concatenate(
                [hot_o * (p == 3 * dz + dx).astype(F32).astype(BF16) for dx in range(3)], axis=0)
            hots.append((start, hot3))
            term = dot(feat[:, start * n : (start + 3) * n], hot3)
            f_o = term if f_o is None else f_o + term
        prod4 = f_c * f_o
        prod = prod4[:ch] + prod4[ch : 2 * ch] + prod4[2 * ch : 3 * ch] + prod4[3 * ch :]
        ph, pl_ = split(prod)
        parts = [l2[k, 0], l2[k, 1], l2[k, 0], ph, pl_, ph]
        if kpad:
            parts.append(jnp.zeros((kpad, n), BF16))
        u = dot(up_t, jnp.concatenate(parts, axis=0))
        sig = 1.0 / (1.0 + jnp.exp(-u))
        hid = u * sig
        raw = jnp.sum(out_col * hid, axis=0, keepdims=True) * alive
        env_grad[i : i + 1] = raw
        e_row = raw * env_row
        e_hi = rounded(e_row)
        e_rows = jnp.where(row_8 == 0, e_hi, jnp.where(row_8 == 1, e_row - e_hi, 0.0)).astype(BF16)
        e_atom = dot_t(e_rows, hot_c)
        energy_ref[k // bx, k % bx : k % bx + 1, :] = e_atom[0:1] + e_atom[1:2]
        d_u = out_col * (alive * env_row) * (sig + hid * (1.0 - sig))
        dh, dl = split(d_u)
        d_join = dot(up3, jnp.concatenate([dh, dl, dh], axis=0))
        dlat_own[k] = d_join[:lat]
        d_prod = jnp.concatenate([d_join[lat:]] * 4, axis=0)
        dch, dcl = split(d_prod * f_o)
        doh, dol = split(d_prod * f_c)
        dfeat[:, i * n : (i + 1) * n] += dot_t(
            jnp.concatenate([dch, dcl], axis=1), jnp.concatenate([hot_c, hot_c], axis=1))
        d_o = jnp.concatenate([doh, dol], axis=1)
        for start, hot3 in hots:
            dfeat[:, start * n : (start + 3) * n] += dot_t(
                d_o, jnp.concatenate([hot3, hot3], axis=1))

    for g in range(0, total, group):
        ids = list(range(g, g + group))
        span = slice(g * n, (g + group) * n)
        dm = []
        for i in ids:
            hot_c = ct[i]
            fh, fl = split(dfeat[:, i * n : (i + 1) * n])
            dm.append(dot(jnp.concatenate([fh, fl], axis=1), jnp.concatenate([hot_c, hot_c], axis=0)))
        dm = join(dm, 1)
        w = wts[:, span]
        dw = dm[:ch]
        for m in range(3):
            piece = dm[(m + 1) * ch : (m + 2) * ch]
            dw = dw + piece * join([harm[m, i : i + 1] for i in ids], 1)
            d_h = jnp.sum(piece * w, axis=0, keepdims=True)
            for t, i in enumerate(ids):
                dharm[m, i : i + 1] = d_h[:, t * n : (t + 1) * n]
        dw = dw * join([rows_live[i : i + 1] for i in ids], 1)
        wh, wl = split(dw)
        parts = [wh, wl, wh]
        if kpad:
            parts.append(jnp.zeros((kpad, group * n), BF16))
        d_lat = dot(env3, jnp.concatenate(parts, axis=0))
        if any(i in interior for i in ids):
            d_lat = d_lat + join(
                [dlat_own[interior[i]] if i in interior else jnp.zeros((lat, n), F32) for i in ids], 1)
        dh, dl = split(d_lat * dsilu[:, span])
        d_r = dot(wr3, jnp.concatenate([dh, dl, dh], axis=0))
        for t, i in enumerate(ids):
            drad[:, i, :] = d_r[:nb, t * n : (t + 1) * n]

    sum_s = drad[0] * sins[0]
    sum_c = drad[0] * coss[0]
    for k in range(1, nb):
        sum_s = sum_s + drad[k] * sins[k]
        sum_c = sum_c + (k + 1.0) * (drad[k] * coss[k])
    env_slope = (-4.0 / CUTOFF) * q * rest
    d_dist = (
        (math.pi / CUTOFF) * sum_c * scale
        - sum_s * scale * inv
        + (sum_s * inv + env_grad[...]) * env_slope
    )
    for m in range(3):
        d_dist = d_dist - dharm[m] * r[m] * (inv * inv)
    gr[...] = jnp.zeros_like(gr)
    for m in range(3):
        d_m = d_dist * harm[m] + dharm[m] * inv
        hi = rounded(d_m)
        gr[:, m, :] = hi
        gr[:, m + 4, :] = d_m - hi

    grad[...] = jnp.zeros_like(grad)
    for i, (a, b) in enumerate(cells):
        g8 = gr[i]
        p = rows_p[i : i + 1]
        at_c = dot_t(jnp.concatenate([g8, jnp.zeros_like(g8)], axis=0).astype(BF16), ct[i])
        stack = [jnp.where(p == off, g8, 0.0) for off in range(9)] + [jnp.zeros_like(g8)]
        at_o = dot_t(jnp.concatenate(stack, axis=0).astype(BF16), ot[i])
        s, y, x = place(a, b)
        grad[s, y, x] -= at_c[:8]
        for off in range(9):
            s, y, x = place(a + off // 3 - 1, b + off % 3 - 1)
            grad[s, y, x] += at_o[8 * off : 8 * off + 8]

    second = []
    for key, s in others_list:
        t = mirror(key)
        copy = pltpu.make_async_remote_copy(
            src_ref=grad.at[s], dst_ref=back.at[t - 1], send_sem=send2.at[s - 1],
            recv_sem=recv2.at[t - 1], device_id=device(key), device_id_type=MESH,
        )
        copy.start()
        second.append(copy)
    for copy in second:
        copy.wait()
    for a in range(bz):
        for b in range(bx):
            acc = grad[0, a, b]
            for s in range(len(others_list)):
                acc = acc + back[s, a, b]
            acc = -(acc[:4] + acc[4:])
            forces_ref[:, a, b, :] = acc[:3]


def solution(mesh):
    nz, nx = mesh.shape["gz"], mesh.shape["xy"]

    def body(coords, species, centers, others, live_count, in_weight, env_weight, up_weight, out_weight):
        _, bz, bx, n = coords.shape
        lat, ch = env_weight.shape
        nb = 8
        spec = (in_weight.shape[0] - nb) // 2
        cells = (bz + 2) * (bx + 2)
        ns = len(neighbours(nz, nx)) - 1
        vmem = lambda shape, dtype=F32: pltpu.VMEM(shape, dtype)
        scratch = [
            vmem((bz, bx, 8, n)),
            vmem((ns, bz, bx, 8, n)),
            vmem((3 * bz, 3 * bx, 16, n), BF16),
            vmem((cells, n, n), BF16),
            vmem((cells, n, n), BF16),
            vmem((cells, n)),
            vmem((cells, n), jnp.int32),
            vmem((4, cells, n)),
            vmem((2 * spec, cells * n)),
            vmem((nb, cells, n)),
            vmem((nb, cells, n)),
            vmem((nb, cells, n)),
            vmem((3, cells, n)),
            vmem((bz * bx, 2, lat, n), BF16),
            vmem((lat, cells * n)),
            vmem((ch, cells * n)),
            vmem((4 * ch, cells * n), BF16),
            vmem((4 * ch, cells * n)),
            vmem((bz * bx, lat, n)),
            vmem((cells, n)),
            vmem((3, cells, n)),
            vmem((nb, cells, n)),
            vmem((cells, 8, n)),
            vmem((ns + 1, bz, bx, 8, n)),
            vmem((ns, bz, bx, 8, n)),
        ] + [pltpu.SemaphoreType.DMA((ns,)) for _ in range(4)]
        specs = [pl.BlockSpec(memory_space=pltpu.VMEM) for _ in range(9)]
        specs[4] = pl.BlockSpec(memory_space=pltpu.SMEM)
        return pl.pallas_call(
            functools.partial(kernel, nz, nx, bz, bx, nb, spec, ch, lat),
            out_shape=(
                jax.ShapeDtypeStruct((bz, bx, n), F32),
                jax.ShapeDtypeStruct((3, bz, bx, n), F32),
            ),
            in_specs=specs,
            out_specs=(pl.BlockSpec(memory_space=pltpu.VMEM), pl.BlockSpec(memory_space=pltpu.VMEM)),
            scratch_shapes=scratch,
            compiler_params=pltpu.CompilerParams(collective_id=0, has_side_effects=True),
        )(coords, species, centers, others, live_count, in_weight, env_weight, up_weight, out_weight[None])

    in_specs = (
        P(None, "gz", "xy", None), P("gz", "xy", None), P("gz", "xy", None), P("gz", "xy", None),
        P("gz", "xy"), P(), P(), P(), P(),
    )
    out_specs = (P("gz", "xy", None), P(None, "gz", "xy", None))
    return jax.shard_map(body, mesh=mesh, in_specs=in_specs, out_specs=out_specs, check_vma=False)
```

```python
import functools
import math

import jax
import jax.numpy as jnp
from jax import lax
from jax.experimental import pallas as pl
from jax.experimental.pallas import tpu as pltpu
from jax.sharding import PartitionSpec as P

SOFTEN = 0.01
CUTOFF = 3.5
F32 = jnp.float32
BF16 = jnp.bfloat16
MESH = pl.DeviceIdType.MESH


def rounded(x):
    return x.astype(BF16).astype(F32)


def split(x):
    high = x.astype(BF16)
    return high, (x - high.astype(F32)).astype(BF16)


def dot(a, b):
    return jnp.dot(a, b, preferred_element_type=F32)


def dot_t(a, b):
    return lax.dot_general(a, b, (((1,), (1,)), ((), ())), preferred_element_type=F32)


def join(parts, axis):
    return parts[0] if len(parts) == 1 else jnp.concatenate(parts, axis=axis)


def neighbours(nz, nx):
    slots = {(0, 0): 0}
    for dz in (-1, 0, 1):
        for dx in (-1, 0, 1):
            slots.setdefault((dz % nz, dx % nx), len(slots))
    return slots


def kernel(
    nz, nx, bz, bx, nb, spec, ch, lat,
    coords_ref, species_ref, centers_ref, others_ref, live_ref, in_ref, env_ref, up_ref, out_ref,
    result_ref,
    own, halo, tab, ct, ot, rows_live, rows_p, geo, xs, sins, coss, rad, harm,
    l2, dsilu, wts, feat, dfeat, dlat_own, env_grad, dharm, drad, gr, grad, back,
    send1, recv1, send2, recv2,
):
    n = coords_ref.shape[-1]
    slots = neighbours(nz, nx)
    me_z, me_x = lax.axis_index("gz"), lax.axis_index("xy")
    others_list = [(key, s) for key, s in slots.items() if s > 0]

    def device(key):
        return (lax.rem(me_z + key[0], nz), lax.rem(me_x + key[1], nx))

    def mirror(key):
        return slots[((-key[0]) % nz, (-key[1]) % nx)]

    barrier = pltpu.get_barrier_semaphore()
    for key, _ in others_list:
        pl.semaphore_signal(barrier, inc=1, device_id=device(key), device_id_type=MESH)

    lane = lax.broadcasted_iota(jnp.int32, (1, n), 1)
    for a in range(bz):
        for b in range(bx):
            alive = (lane < live_ref[a, b]).astype(F32)
            own[a, b] = jnp.concatenate(
                [
                    coords_ref[:, a, b, :],
                    species_ref[a, b : b + 1, :].astype(F32),
                    centers_ref[a, b : b + 1, :].astype(F32),
                    others_ref[a, b : b + 1, :].astype(F32),
                    alive,
                    jnp.zeros((1, n), F32),
                ],
                axis=0,
            )
    pl.semaphore_wait(barrier, len(others_list))
    first = []
    for key, s in others_list:
        t = mirror(key)
        copy = pltpu.make_async_remote_copy(
            src_ref=own, dst_ref=halo.at[t - 1], send_sem=send1.at[s - 1],
            recv_sem=recv1.at[t - 1], device_id=device(key), device_id_type=MESH,
        )
        copy.start()
        first.append(copy)

    w_in = in_ref[...]
    w_hi = rounded(w_in)
    w_lo = w_in - w_hi
    w_rows = jnp.concatenate(
        [w_hi[:nb], w_lo[:nb], w_hi[:nb], w_hi[nb:], w_lo[nb:],
         jnp.zeros((lat - 3 * nb - 4 * spec, lat), F32)], axis=0)
    kin = (3 * nb + 4 * spec + 15) // 16 * 16
    in_t = w_rows.T.astype(BF16)[:, :kin]
    pad8 = jnp.zeros((nb, lat), F32)
    wr_hi = jnp.concatenate([w_hi[:nb], pad8], axis=0).astype(BF16)
    wr_lo = jnp.concatenate([w_lo[:nb], pad8], axis=0).astype(BF16)
    wr3 = jnp.concatenate([wr_hi, wr_hi, wr_lo], axis=1)
    env_t = env_ref[...]
    et_hi = rounded(env_t)
    et_lo = env_t - et_hi
    env_t3 = jnp.concatenate([et_hi, et_hi, et_lo], axis=1).astype(BF16)
    kpad = -(3 * ch) % lat
    env3 = jnp.concatenate(
        [et_hi, et_hi, et_lo] + ([jnp.zeros((kpad, lat), F32)] if kpad else []), axis=0
    ).T.astype(BF16)
    up = up_ref[...]
    up_hi = rounded(up)
    up_lo = up - up_hi
    up3 = jnp.concatenate([up_hi, up_hi, up_lo], axis=1).astype(BF16)
    up_t = jnp.concatenate(
        [x.T.astype(BF16) for x in (up_hi[:lat], up_hi[:lat], up_lo[:lat])]
        + [jnp.concatenate(
            [up_hi[lat:], up_hi[lat:], up_lo[lat:]]
            + ([jnp.zeros((kpad, lat), F32)] if kpad else []), axis=0).T.astype(BF16)],
        axis=1)
    out_col = jnp.broadcast_to(out_ref[...], (n, lat)).T

    for copy in first:
        copy.wait()

    def place(a, b):
        return slots[((a // bz - 1) % nz, (b // bx - 1) % nx)], a % bz, b % bx

    def block(a, b):
        s, i, j = place(a, b)
        return own[i, j] if s == 0 else halo[s - 1, i, j]

    window_z = range(bz - 2, 2 * bz + 2)
    window_x = range(bx - 2, 2 * bx + 2)
    for a in window_z:
        for b in window_x:
            part = block(a, b)
            hi = rounded(part)
            tab[a, b] = jnp.concatenate([hi, part - hi], axis=0).astype(BF16)

    cells = [(a, b) for a in range(bz - 1, 2 * bz + 1) for b in range(bx - 1, 2 * bx + 1)]
    cx = bx + 2
    total = len(cells)
    row_n = lax.broadcasted_iota(jnp.int32, (n, n), 0)
    row_s = lax.broadcasted_iota(jnp.int32, (spec, n), 0).astype(F32)
    for i, (a, b) in enumerate(cells):
        part = block(a, b)
        c = part[4:5].astype(jnp.int32)
        o = part[5:6].astype(jnp.int32)
        p = o >> 7
        hot_c = (row_n == c).astype(F32).astype(BF16)
        hot_o = (row_n == (o & 127)).astype(F32).astype(BF16)
        ct[i] = hot_c
        ot[i] = hot_o
        at_c = dot(tab[a, b], hot_c)
        at_c = at_c[:8] + at_c[8:]
        around = jnp.concatenate(
            [tab[a + dz, b + dx] for dz in (-1, 0, 1) for dx in (-1, 0, 1)], axis=0)
        got = dot(around, hot_o)
        at_o = jnp.zeros((8, n), F32)
        for off in range(9):
            at_o = jnp.where(p == off, got[16 * off : 16 * off + 8] + got[16 * off + 8 : 16 * off + 16], at_o)
        diff = at_o - at_c
        up3_ = (p >= 3).astype(jnp.int32) + (p >= 6).astype(jnp.int32)
        geo[0, i : i + 1] = diff[0:1] + (up3_ - 1).astype(F32)
        geo[1, i : i + 1] = diff[1:2] + (p - 3 * up3_ - 1).astype(F32)
        geo[2, i : i + 1] = diff[2:3]
        xs[:spec, i * n : (i + 1) * n] = (row_s == at_c[3:4]).astype(F32)
        xs[spec:, i * n : (i + 1) * n] = (row_s == at_o[3:4]).astype(F32)
        rows_live[i : i + 1] = part[6:7]
        rows_p[i : i + 1] = p

    r = [geo[m] for m in range(3)]
    dist = jnp.sqrt(r[0] * r[0] + r[1] * r[1] + r[2] * r[2] + SOFTEN)
    inv = 1.0 / dist
    q = dist / CUTOFF
    rest = 1.0 - q * q
    envelope = rest * rest
    scale = inv * envelope
    s1 = jnp.sin(math.pi * q)
    c1 = jnp.cos(math.pi * q)
    s0, c0, sk, ck = jnp.zeros_like(s1), jnp.ones_like(c1), s1, c1
    for k in range(nb):
        sins[k] = sk
        coss[k] = ck
        rad[k] = sk * scale
        s0, sk = sk, 2.0 * c1 * sk - s0
        c0, ck = ck, 2.0 * c1 * ck - c0
    for m in range(3):
        harm[m] = r[m] * inv
    env_grad[...] = jnp.zeros_like(env_grad)
    geo[3] = envelope

    interior = {}
    for i, (a, b) in enumerate(cells):
        if bz <= a < 2 * bz and bx <= b < 2 * bx:
            interior[i] = (a - bz) * bx + (b - bx)

    group = 2 if total % 2 == 0 else 1
    for g in range(0, total, group):
        ids = list(range(g, g + group))
        span = slice(g * n, (g + group) * n)
        radial = join([rad[:, i, :] for i in ids], 1)
        rh = rounded(radial)
        x_s = xs[:, span]
        parts = [rh, rh, radial - rh, x_s, x_s]
        fill = kin - 3 * nb - 4 * spec
        if fill:
            parts.append(jnp.zeros((fill, group * n), F32))
        pre = dot(in_t, jnp.concatenate(parts, axis=0).astype(BF16))
        sig = 1.0 / (1.0 + jnp.exp(-pre))
        latent = pre * sig
        dsilu[:, span] = sig + latent * (1.0 - sig)
        lh, ll = split(latent)
        for t, i in enumerate(ids):
            if i in interior:
                l2[interior[i], 0] = lh[:, t * n : (t + 1) * n]
                l2[interior[i], 1] = ll[:, t * n : (t + 1) * n]
        alive = join([rows_live[i : i + 1] for i in ids], 1)
        w = dot(env_t3, jnp.concatenate([lh, ll, lh], axis=0)) * alive
        wts[:, span] = w
        msgs = jnp.concatenate(
            [w] + [w * join([harm[m, i : i + 1] for i in ids], 1) for m in range(3)], axis=0)
        mh, ml = split(msgs)
        for t, i in enumerate(ids):
            cut = slice(t * n, (t + 1) * n)
            hot_c = ct[i]
            feat[:, i * n : (i + 1) * n] = dot_t(
                jnp.concatenate([mh[:, cut], ml[:, cut]], axis=1),
                jnp.concatenate([hot_c, hot_c], axis=1)).astype(BF16)

    dfeat[...] = jnp.zeros_like(dfeat)
    row_8 = lax.broadcasted_iota(jnp.int32, (16, n), 0)
    for i, k in interior.items():
        hot_c, hot_o = ct[i], ot[i]
        p = rows_p[i : i + 1]
        env_row = geo[3, i : i + 1]
        alive = rows_live[i : i + 1]
        f_c = dot(feat[:, i * n : (i + 1) * n], hot_c)
        f_o = None
        hots = []
        for dz in range(3):
            start = i + (dz - 1) * cx - 1
            hot3 = jnp.concatenate(
                [hot_o * (p == 3 * dz + dx).astype(F32).astype(BF16) for dx in range(3)], axis=0)
            hots.append((start, hot3))
            term = dot(feat[:, start * n : (start + 3) * n], hot3)
            f_o = term if f_o is None else f_o + term
        prod4 = f_c * f_o
        prod = prod4[:ch] + prod4[ch : 2 * ch] + prod4[2 * ch : 3 * ch] + prod4[3 * ch :]
        ph, pl_ = split(prod)
        parts = [l2[k, 0], l2[k, 1], l2[k, 0], ph, pl_, ph]
        if kpad:
            parts.append(jnp.zeros((kpad, n), BF16))
        u = dot(up_t, jnp.concatenate(parts, axis=0))
        sig = 1.0 / (1.0 + jnp.exp(-u))
        hid = u * sig
        raw = jnp.sum(out_col * hid, axis=0, keepdims=True) * alive
        env_grad[i : i + 1] = raw
        e_row = raw * env_row
        e_hi = rounded(e_row)
        e_rows = jnp.where(row_8 == 0, e_hi, jnp.where(row_8 == 1, e_row - e_hi, 0.0)).astype(BF16)
        e_atom = dot_t(e_rows, hot_c)
        result_ref[3, k // bx, k % bx : k % bx + 1, :] = e_atom[0:1] + e_atom[1:2]
        d_u = out_col * (alive * env_row) * (sig + hid * (1.0 - sig))
        dh, dl = split(d_u)
        d_join = dot(up3, jnp.concatenate([dh, dl, dh], axis=0))
        dlat_own[k] = d_join[:lat]
        d_prod = jnp.concatenate([d_join[lat:]] * 4, axis=0)
        dch, dcl = split(d_prod * f_o)
        doh, dol = split(d_prod * f_c)
        dfeat[:, i * n : (i + 1) * n] += dot_t(
            jnp.concatenate([dch, dcl], axis=1), jnp.concatenate([hot_c, hot_c], axis=1))
        d_o = jnp.concatenate([doh, dol], axis=1)
        for start, hot3 in hots:
            dfeat[:, start * n : (start + 3) * n] += dot_t(
                d_o, jnp.concatenate([hot3, hot3], axis=1))

    for g in range(0, total, group):
        ids = list(range(g, g + group))
        span = slice(g * n, (g + group) * n)
        dm = []
        for i in ids:
            hot_c = ct[i]
            fh, fl = split(dfeat[:, i * n : (i + 1) * n])
            dm.append(dot(jnp.concatenate([fh, fl], axis=1), jnp.concatenate([hot_c, hot_c], axis=0)))
        dm = join(dm, 1)
        w = wts[:, span]
        dw = dm[:ch]
        for m in range(3):
            piece = dm[(m + 1) * ch : (m + 2) * ch]
            dw = dw + piece * join([harm[m, i : i + 1] for i in ids], 1)
            d_h = jnp.sum(piece * w, axis=0, keepdims=True)
            for t, i in enumerate(ids):
                dharm[m, i : i + 1] = d_h[:, t * n : (t + 1) * n]
        dw = dw * join([rows_live[i : i + 1] for i in ids], 1)
        wh, wl = split(dw)
        parts = [wh, wl, wh]
        if kpad:
            parts.append(jnp.zeros((kpad, group * n), BF16))
        d_lat = dot(env3, jnp.concatenate(parts, axis=0))
        if any(i in interior for i in ids):
            d_lat = d_lat + join(
                [dlat_own[interior[i]] if i in interior else jnp.zeros((lat, n), F32) for i in ids], 1)
        dh, dl = split(d_lat * dsilu[:, span])
        d_r = dot(wr3, jnp.concatenate([dh, dl, dh], axis=0))
        for t, i in enumerate(ids):
            drad[:, i, :] = d_r[:nb, t * n : (t + 1) * n]

    sum_s = drad[0] * sins[0]
    sum_c = drad[0] * coss[0]
    for k in range(1, nb):
        sum_s = sum_s + drad[k] * sins[k]
        sum_c = sum_c + (k + 1.0) * (drad[k] * coss[k])
    env_slope = (-4.0 / CUTOFF) * q * rest
    d_dist = (
        (math.pi / CUTOFF) * sum_c * scale
        - sum_s * scale * inv
        + (sum_s * inv + env_grad[...]) * env_slope
    )
    for m in range(3):
        d_dist = d_dist - dharm[m] * r[m] * (inv * inv)
    gr[...] = jnp.zeros_like(gr)
    for m in range(3):
        d_m = d_dist * harm[m] + dharm[m] * inv
        hi = rounded(d_m)
        gr[:, m, :] = hi
        gr[:, m + 4, :] = d_m - hi

    grad[...] = jnp.zeros_like(grad)
    for i, (a, b) in enumerate(cells):
        g8 = gr[i]
        p = rows_p[i : i + 1]
        at_c = dot_t(jnp.concatenate([g8, jnp.zeros_like(g8)], axis=0).astype(BF16), ct[i])
        stack = [jnp.where(p == off, g8, 0.0) for off in range(9)] + [jnp.zeros_like(g8)]
        at_o = dot_t(jnp.concatenate(stack, axis=0).astype(BF16), ot[i])
        s, y, x = place(a, b)
        grad[s, y, x] -= at_c[:8]
        for off in range(9):
            s, y, x = place(a + off // 3 - 1, b + off % 3 - 1)
            grad[s, y, x] += at_o[8 * off : 8 * off + 8]

    second = []
    for key, s in others_list:
        t = mirror(key)
        copy = pltpu.make_async_remote_copy(
            src_ref=grad.at[s], dst_ref=back.at[t - 1], send_sem=send2.at[s - 1],
            recv_sem=recv2.at[t - 1], device_id=device(key), device_id_type=MESH,
        )
        copy.start()
        second.append(copy)
    for copy in second:
        copy.wait()
    for a in range(bz):
        for b in range(bx):
            acc = grad[0, a, b]
            for s in range(len(others_list)):
                acc = acc + back[s, a, b]
            acc = -(acc[:4] + acc[4:])
            result_ref[:3, a, b, :] = acc[:3]


def solution(mesh):
    nz, nx = mesh.shape["gz"], mesh.shape["xy"]

    def body(coords, species, centers, others, live_count, in_weight, env_weight, up_weight, out_weight):
        _, bz, bx, n = coords.shape
        lat, ch = env_weight.shape
        nb = 8
        spec = (in_weight.shape[0] - nb) // 2
        cells = (bz + 2) * (bx + 2)
        ns = len(neighbours(nz, nx)) - 1
        vmem = lambda shape, dtype=F32: pltpu.VMEM(shape, dtype)
        scratch = [
            vmem((bz, bx, 8, n)),
            vmem((ns, bz, bx, 8, n)),
            vmem((3 * bz, 3 * bx, 16, n), BF16),
            vmem((cells, n, n), BF16),
            vmem((cells, n, n), BF16),
            vmem((cells, n)),
            vmem((cells, n), jnp.int32),
            vmem((4, cells, n)),
            vmem((2 * spec, cells * n)),
            vmem((nb, cells, n)),
            vmem((nb, cells, n)),
            vmem((nb, cells, n)),
            vmem((3, cells, n)),
            vmem((bz * bx, 2, lat, n), BF16),
            vmem((lat, cells * n)),
            vmem((ch, cells * n)),
            vmem((4 * ch, cells * n), BF16),
            vmem((4 * ch, cells * n)),
            vmem((bz * bx, lat, n)),
            vmem((cells, n)),
            vmem((3, cells, n)),
            vmem((nb, cells, n)),
            vmem((cells, 8, n)),
            vmem((ns + 1, bz, bx, 8, n)),
            vmem((ns, bz, bx, 8, n)),
        ] + [pltpu.SemaphoreType.DMA((ns,)) for _ in range(4)]
        specs = [pl.BlockSpec(memory_space=pltpu.VMEM) for _ in range(9)]
        specs[4] = pl.BlockSpec(memory_space=pltpu.SMEM)
        result = pl.pallas_call(
            functools.partial(kernel, nz, nx, bz, bx, nb, spec, ch, lat),
            out_shape=jax.ShapeDtypeStruct((4, bz, bx, n), F32),
            in_specs=specs,
            out_specs=pl.BlockSpec(memory_space=pltpu.VMEM),
            scratch_shapes=scratch,
            compiler_params=pltpu.CompilerParams(collective_id=0, has_side_effects=True),
        )(coords, species, centers, others, live_count, in_weight, env_weight.T, up_weight, out_weight[None])
        return result[3], result[:3]

    in_specs = (
        P(None, "gz", "xy", None), P("gz", "xy", None), P("gz", "xy", None), P("gz", "xy", None),
        P("gz", "xy"), P(), P(), P(), P(),
    )
    out_specs = (P("gz", "xy", None), P(None, "gz", "xy", None))
    return jax.shard_map(body, mesh=mesh, in_specs=in_specs, out_specs=out_specs, check_vma=False)
```

```python
import functools
import math

import jax
import jax.numpy as jnp
from jax import lax
from jax.experimental import pallas as pl
from jax.experimental.pallas import tpu as pltpu
from jax.sharding import PartitionSpec as P

SOFTEN = 0.01
CUTOFF = 3.5
F32 = jnp.float32
BF16 = jnp.bfloat16
MESH = pl.DeviceIdType.MESH


def rounded(x):
    return x.astype(BF16).astype(F32)


def split(x):
    high = x.astype(BF16)
    return high, (x - high.astype(F32)).astype(BF16)


def dot(a, b):
    return jnp.dot(a, b, preferred_element_type=F32)


def dot_t(a, b):
    return lax.dot_general(a, b, (((1,), (1,)), ((), ())), preferred_element_type=F32)


def join(parts, axis):
    return parts[0] if len(parts) == 1 else jnp.concatenate(parts, axis=axis)


def neighbours(nz, nx):
    slots = {(0, 0): 0}
    for dz in (-1, 0, 1):
        for dx in (-1, 0, 1):
            slots.setdefault((dz % nz, dx % nx), len(slots))
    return slots


def kernel(
    nz, nx, bz, bx, nb, spec, ch, lat,
    coords_hbm, species_hbm, centers_hbm, others_hbm, live_hbm, in_hbm, env_hbm, up_hbm, out_hbm,
    result_ref,
    coords_ref, species_ref, centers_ref, others_ref, live_ref, in_ref, env_ref, up_ref, out_ref,
    own, halo, tab, ct, ot, rows_live, rows_p, geo, xs, sins, coss, rad, harm,
    l2, dsilu, wts, feat, dfeat, dlat_own, env_grad, dharm, drad, gr, grad, back,
    send1, recv1, send2, recv2, load_sem,
):
    n = coords_ref.shape[-1]
    slots = neighbours(nz, nx)
    me_z, me_x = lax.axis_index("gz"), lax.axis_index("xy")
    others_list = [(key, s) for key, s in slots.items() if s > 0]

    def device(key):
        return (lax.rem(me_z + key[0], nz), lax.rem(me_x + key[1], nx))

    def mirror(key):
        return slots[((-key[0]) % nz, (-key[1]) % nx)]

    barrier = pltpu.get_barrier_semaphore()
    for key, _ in others_list:
        pl.semaphore_signal(barrier, inc=1, device_id=device(key), device_id_type=MESH)

    loads = [
        pltpu.make_async_copy(source, target, load_sem.at[k])
        for k, (source, target) in enumerate([
            (coords_hbm, coords_ref), (species_hbm, species_ref), (centers_hbm, centers_ref),
            (others_hbm, others_ref), (live_hbm, live_ref), (in_hbm, in_ref), (env_hbm, env_ref),
            (up_hbm, up_ref), (out_hbm, out_ref)])
    ]
    for load in loads:
        load.start()
    for load in loads[:5]:
        load.wait()
    lane = lax.broadcasted_iota(jnp.int32, (1, n), 1)
    for a in range(bz):
        for b in range(bx):
            alive = (lane < live_ref[a : a + 1, b : b + 1]).astype(F32)
            own[a, b] = jnp.concatenate(
                [
                    coords_ref[:, a, b, :],
                    species_ref[a, b : b + 1, :].astype(F32),
                    centers_ref[a, b : b + 1, :].astype(F32),
                    others_ref[a, b : b + 1, :].astype(F32),
                    alive,
                    jnp.zeros((1, n), F32),
                ],
                axis=0,
            )
    pl.semaphore_wait(barrier, len(others_list))
    first = []
    for key, s in others_list:
        t = mirror(key)
        copy = pltpu.make_async_remote_copy(
            src_ref=own, dst_ref=halo.at[t - 1], send_sem=send1.at[s - 1],
            recv_sem=recv1.at[t - 1], device_id=device(key), device_id_type=MESH,
        )
        copy.start()
        first.append(copy)

    for load in loads[5:]:
        load.wait()
    w_in = in_ref[...]
    w_hi = rounded(w_in)
    w_lo = w_in - w_hi
    w_rows = jnp.concatenate(
        [w_hi[:nb], w_lo[:nb], w_hi[:nb], w_hi[nb:], w_lo[nb:],
         jnp.zeros((lat - 3 * nb - 4 * spec, lat), F32)], axis=0)
    kin = (3 * nb + 4 * spec + 15) // 16 * 16
    in_t = w_rows.T.astype(BF16)[:, :kin]
    pad8 = jnp.zeros((nb, lat), F32)
    wr_hi = jnp.concatenate([w_hi[:nb], pad8], axis=0).astype(BF16)
    wr_lo = jnp.concatenate([w_lo[:nb], pad8], axis=0).astype(BF16)
    wr3 = jnp.concatenate([wr_hi, wr_hi, wr_lo], axis=1)
    env_t = env_ref[...]
    et_hi = rounded(env_t)
    et_lo = env_t - et_hi
    env_t3 = jnp.concatenate([et_hi, et_hi, et_lo], axis=1).astype(BF16)
    kpad = -(3 * ch) % lat
    env3 = jnp.concatenate(
        [et_hi, et_hi, et_lo] + ([jnp.zeros((kpad, lat), F32)] if kpad else []), axis=0
    ).T.astype(BF16)
    up = up_ref[...]
    up_hi = rounded(up)
    up_lo = up - up_hi
    up3 = jnp.concatenate([up_hi, up_hi, up_lo], axis=1).astype(BF16)
    up_t = jnp.concatenate(
        [x.T.astype(BF16) for x in (up_hi[:lat], up_hi[:lat], up_lo[:lat])]
        + [jnp.concatenate(
            [up_hi[lat:], up_hi[lat:], up_lo[lat:]]
            + ([jnp.zeros((kpad, lat), F32)] if kpad else []), axis=0).T.astype(BF16)],
        axis=1)
    out_col = jnp.broadcast_to(out_ref[...], (n, lat)).T

    for copy in first:
        copy.wait()

    def place(a, b):
        return slots[((a // bz - 1) % nz, (b // bx - 1) % nx)], a % bz, b % bx

    def block(a, b):
        s, i, j = place(a, b)
        return own[i, j] if s == 0 else halo[s - 1, i, j]

    window_z = range(bz - 2, 2 * bz + 2)
    window_x = range(bx - 2, 2 * bx + 2)
    for a in window_z:
        for b in window_x:
            part = block(a, b)
            hi = rounded(part)
            tab[a, b] = jnp.concatenate([hi, part - hi], axis=0).astype(BF16)

    cells = [(a, b) for a in range(bz - 1, 2 * bz + 1) for b in range(bx - 1, 2 * bx + 1)]
    cx = bx + 2
    total = len(cells)
    row_n = lax.broadcasted_iota(jnp.int32, (n, n), 0)
    row_s = lax.broadcasted_iota(jnp.int32, (spec, n), 0).astype(F32)
    for i, (a, b) in enumerate(cells):
        part = block(a, b)
        c = part[4:5].astype(jnp.int32)
        o = part[5:6].astype(jnp.int32)
        p = o >> 7
        hot_c = (row_n == c).astype(F32).astype(BF16)
        hot_o = (row_n == (o & 127)).astype(F32).astype(BF16)
        ct[i] = hot_c
        ot[i] = hot_o
        at_c = dot(tab[a, b], hot_c)
        at_c = at_c[:8] + at_c[8:]
        around = jnp.concatenate(
            [tab[a + dz, b + dx] for dz in (-1, 0, 1) for dx in (-1, 0, 1)], axis=0)
        got = dot(around, hot_o)
        at_o = jnp.zeros((8, n), F32)
        for off in range(9):
            at_o = jnp.where(p == off, got[16 * off : 16 * off + 8] + got[16 * off + 8 : 16 * off + 16], at_o)
        diff = at_o - at_c
        up3_ = (p >= 3).astype(jnp.int32) + (p >= 6).astype(jnp.int32)
        geo[0, i : i + 1] = diff[0:1] + (up3_ - 1).astype(F32)
        geo[1, i : i + 1] = diff[1:2] + (p - 3 * up3_ - 1).astype(F32)
        geo[2, i : i + 1] = diff[2:3]
        xs[:spec, i * n : (i + 1) * n] = (row_s == at_c[3:4]).astype(F32)
        xs[spec:, i * n : (i + 1) * n] = (row_s == at_o[3:4]).astype(F32)
        rows_live[i : i + 1] = part[6:7]
        rows_p[i : i + 1] = p

    r = [geo[m] for m in range(3)]
    dist = jnp.sqrt(r[0] * r[0] + r[1] * r[1] + r[2] * r[2] + SOFTEN)
    inv = 1.0 / dist
    q = dist / CUTOFF
    rest = 1.0 - q * q
    envelope = rest * rest
    scale = inv * envelope
    s1 = jnp.sin(math.pi * q)
    c1 = jnp.cos(math.pi * q)
    s0, c0, sk, ck = jnp.zeros_like(s1), jnp.ones_like(c1), s1, c1
    for k in range(nb):
        sins[k] = sk
        coss[k] = ck
        rad[k] = sk * scale
        s0, sk = sk, 2.0 * c1 * sk - s0
        c0, ck = ck, 2.0 * c1 * ck - c0
    for m in range(3):
        harm[m] = r[m] * inv
    env_grad[...] = jnp.zeros_like(env_grad)
    geo[3] = envelope

    interior = {}
    for i, (a, b) in enumerate(cells):
        if bz <= a < 2 * bz and bx <= b < 2 * bx:
            interior[i] = (a - bz) * bx + (b - bx)

    group = 2 if total % 2 == 0 else 1
    for g in range(0, total, group):
        ids = list(range(g, g + group))
        span = slice(g * n, (g + group) * n)
        radial = join([rad[:, i, :] for i in ids], 1)
        rh = rounded(radial)
        x_s = xs[:, span]
        parts = [rh, rh, radial - rh, x_s, x_s]
        fill = kin - 3 * nb - 4 * spec
        if fill:
            parts.append(jnp.zeros((fill, group * n), F32))
        pre = dot(in_t, jnp.concatenate(parts, axis=0).astype(BF16))
        sig = 1.0 / (1.0 + jnp.exp(-pre))
        latent = pre * sig
        dsilu[:, span] = sig + latent * (1.0 - sig)
        lh, ll = split(latent)
        for t, i in enumerate(ids):
            if i in interior:
                l2[interior[i], 0] = lh[:, t * n : (t + 1) * n]
                l2[interior[i], 1] = ll[:, t * n : (t + 1) * n]
        alive = join([rows_live[i : i + 1] for i in ids], 1)
        w = dot(env_t3, jnp.concatenate([lh, ll, lh], axis=0)) * alive
        wts[:, span] = w
        msgs = jnp.concatenate(
            [w] + [w * join([harm[m, i : i + 1] for i in ids], 1) for m in range(3)], axis=0)
        mh, ml = split(msgs)
        for t, i in enumerate(ids):
            cut = slice(t * n, (t + 1) * n)
            hot_c = ct[i]
            feat[:, i * n : (i + 1) * n] = dot_t(
                jnp.concatenate([mh[:, cut], ml[:, cut]], axis=1),
                jnp.concatenate([hot_c, hot_c], axis=1)).astype(BF16)

    dfeat[...] = jnp.zeros_like(dfeat)
    row_8 = lax.broadcasted_iota(jnp.int32, (16, n), 0)
    for i, k in interior.items():
        hot_c, hot_o = ct[i], ot[i]
        p = rows_p[i : i + 1]
        env_row = geo[3, i : i + 1]
        alive = rows_live[i : i + 1]
        f_c = dot(feat[:, i * n : (i + 1) * n], hot_c)
        f_o = None
        hots = []
        for dz in range(3):
            start = i + (dz - 1) * cx - 1
            hot3 = jnp.concatenate(
                [hot_o * (p == 3 * dz + dx).astype(F32).astype(BF16) for dx in range(3)], axis=0)
            hots.append((start, hot3))
            term = dot(feat[:, start * n : (start + 3) * n], hot3)
            f_o = term if f_o is None else f_o + term
        prod4 = f_c * f_o
        prod = prod4[:ch] + prod4[ch : 2 * ch] + prod4[2 * ch : 3 * ch] + prod4[3 * ch :]
        ph, pl_ = split(prod)
        parts = [l2[k, 0], l2[k, 1], l2[k, 0], ph, pl_, ph]
        if kpad:
            parts.append(jnp.zeros((kpad, n), BF16))
        u = dot(up_t, jnp.concatenate(parts, axis=0))
        sig = 1.0 / (1.0 + jnp.exp(-u))
        hid = u * sig
        raw = jnp.sum(out_col * hid, axis=0, keepdims=True) * alive
        env_grad[i : i + 1] = raw
        e_row = raw * env_row
        e_hi = rounded(e_row)
        e_rows = jnp.where(row_8 == 0, e_hi, jnp.where(row_8 == 1, e_row - e_hi, 0.0)).astype(BF16)
        e_atom = dot_t(e_rows, hot_c)
        result_ref[3, k // bx, k % bx : k % bx + 1, :] = e_atom[0:1] + e_atom[1:2]
        d_u = out_col * (alive * env_row) * (sig + hid * (1.0 - sig))
        dh, dl = split(d_u)
        d_join = dot(up3, jnp.concatenate([dh, dl, dh], axis=0))
        dlat_own[k] = d_join[:lat]
        d_prod = jnp.concatenate([d_join[lat:]] * 4, axis=0)
        dch, dcl = split(d_prod * f_o)
        doh, dol = split(d_prod * f_c)
        dfeat[:, i * n : (i + 1) * n] += dot_t(
            jnp.concatenate([dch, dcl], axis=1), jnp.concatenate([hot_c, hot_c], axis=1))
        d_o = jnp.concatenate([doh, dol], axis=1)
        for start, hot3 in hots:
            dfeat[:, start * n : (start + 3) * n] += dot_t(
                d_o, jnp.concatenate([hot3, hot3], axis=1))

    for g in range(0, total, group):
        ids = list(range(g, g + group))
        span = slice(g * n, (g + group) * n)
        dm = []
        for i in ids:
            hot_c = ct[i]
            fh, fl = split(dfeat[:, i * n : (i + 1) * n])
            dm.append(dot(jnp.concatenate([fh, fl], axis=1), jnp.concatenate([hot_c, hot_c], axis=0)))
        dm = join(dm, 1)
        w = wts[:, span]
        dw = dm[:ch]
        for m in range(3):
            piece = dm[(m + 1) * ch : (m + 2) * ch]
            dw = dw + piece * join([harm[m, i : i + 1] for i in ids], 1)
            d_h = jnp.sum(piece * w, axis=0, keepdims=True)
            for t, i in enumerate(ids):
                dharm[m, i : i + 1] = d_h[:, t * n : (t + 1) * n]
        dw = dw * join([rows_live[i : i + 1] for i in ids], 1)
        wh, wl = split(dw)
        parts = [wh, wl, wh]
        if kpad:
            parts.append(jnp.zeros((kpad, group * n), BF16))
        d_lat = dot(env3, jnp.concatenate(parts, axis=0))
        if any(i in interior for i in ids):
            d_lat = d_lat + join(
                [dlat_own[interior[i]] if i in interior else jnp.zeros((lat, n), F32) for i in ids], 1)
        dh, dl = split(d_lat * dsilu[:, span])
        d_r = dot(wr3, jnp.concatenate([dh, dl, dh], axis=0))
        for t, i in enumerate(ids):
            drad[:, i, :] = d_r[:nb, t * n : (t + 1) * n]

    sum_s = drad[0] * sins[0]
    sum_c = drad[0] * coss[0]
    for k in range(1, nb):
        sum_s = sum_s + drad[k] * sins[k]
        sum_c = sum_c + (k + 1.0) * (drad[k] * coss[k])
    env_slope = (-4.0 / CUTOFF) * q * rest
    d_dist = (
        (math.pi / CUTOFF) * sum_c * scale
        - sum_s * scale * inv
        + (sum_s * inv + env_grad[...]) * env_slope
    )
    for m in range(3):
        d_dist = d_dist - dharm[m] * r[m] * (inv * inv)
    gr[...] = jnp.zeros_like(gr)
    for m in range(3):
        d_m = d_dist * harm[m] + dharm[m] * inv
        hi = rounded(d_m)
        gr[:, m, :] = hi
        gr[:, m + 4, :] = d_m - hi

    grad[...] = jnp.zeros_like(grad)
    for i, (a, b) in enumerate(cells):
        g8 = gr[i]
        p = rows_p[i : i + 1]
        at_c = dot_t(jnp.concatenate([g8, jnp.zeros_like(g8)], axis=0).astype(BF16), ct[i])
        stack = [jnp.where(p == off, g8, 0.0) for off in range(9)] + [jnp.zeros_like(g8)]
        at_o = dot_t(jnp.concatenate(stack, axis=0).astype(BF16), ot[i])
        s, y, x = place(a, b)
        grad[s, y, x] -= at_c[:8]
        for off in range(9):
            s, y, x = place(a + off // 3 - 1, b + off % 3 - 1)
            grad[s, y, x] += at_o[8 * off : 8 * off + 8]

    second = []
    for key, s in others_list:
        t = mirror(key)
        copy = pltpu.make_async_remote_copy(
            src_ref=grad.at[s], dst_ref=back.at[t - 1], send_sem=send2.at[s - 1],
            recv_sem=recv2.at[t - 1], device_id=device(key), device_id_type=MESH,
        )
        copy.start()
        second.append(copy)
    for copy in second:
        copy.wait()
    for a in range(bz):
        for b in range(bx):
            acc = grad[0, a, b]
            for s in range(len(others_list)):
                acc = acc + back[s, a, b]
            acc = -(acc[:4] + acc[4:])
            result_ref[:3, a, b, :] = acc[:3]


def solution(mesh):
    nz, nx = mesh.shape["gz"], mesh.shape["xy"]

    def body(coords, species, centers, others, live_count, in_weight, env_weight, up_weight, out_weight):
        _, bz, bx, n = coords.shape
        lat, ch = env_weight.shape
        nb = 8
        spec = (in_weight.shape[0] - nb) // 2
        cells = (bz + 2) * (bx + 2)
        ns = len(neighbours(nz, nx)) - 1
        vmem = lambda shape, dtype=F32: pltpu.VMEM(shape, dtype)
        args = (coords, species, centers, others, live_count, in_weight, env_weight.T, up_weight,
                out_weight[None])
        scratch = [vmem(x.shape, x.dtype) for x in args] + [
            vmem((bz, bx, 8, n)),
            vmem((ns, bz, bx, 8, n)),
            vmem((3 * bz, 3 * bx, 16, n), BF16),
            vmem((cells, n, n), BF16),
            vmem((cells, n, n), BF16),
            vmem((cells, n)),
            vmem((cells, n), jnp.int32),
            vmem((4, cells, n)),
            vmem((2 * spec, cells * n)),
            vmem((nb, cells, n)),
            vmem((nb, cells, n)),
            vmem((nb, cells, n)),
            vmem((3, cells, n)),
            vmem((bz * bx, 2, lat, n), BF16),
            vmem((lat, cells * n)),
            vmem((ch, cells * n)),
            vmem((4 * ch, cells * n), BF16),
            vmem((4 * ch, cells * n)),
            vmem((bz * bx, lat, n)),
            vmem((cells, n)),
            vmem((3, cells, n)),
            vmem((nb, cells, n)),
            vmem((cells, 8, n)),
            vmem((ns + 1, bz, bx, 8, n)),
            vmem((ns, bz, bx, 8, n)),
        ] + [pltpu.SemaphoreType.DMA((ns,)) for _ in range(4)]
        scratch.append(pltpu.SemaphoreType.DMA((len(args),)))
        specs = [pl.BlockSpec(memory_space=pl.ANY) for _ in args]
        result = pl.pallas_call(
            functools.partial(kernel, nz, nx, bz, bx, nb, spec, ch, lat),
            out_shape=pltpu.VMEM((4, bz, bx, n), F32),
            in_specs=specs,
            out_specs=pl.BlockSpec(memory_space=pltpu.VMEM),
            scratch_shapes=scratch,
            compiler_params=pltpu.CompilerParams(collective_id=0, has_side_effects=True),
        )(*args)
        return result[3], result[:3]

    in_specs = (
        P(None, "gz", "xy", None), P("gz", "xy", None), P("gz", "xy", None), P("gz", "xy", None),
        P("gz", "xy"), P(), P(), P(), P(),
    )
    out_specs = (P("gz", "xy", None), P(None, "gz", "xy", None))
    return jax.shard_map(body, mesh=mesh, in_specs=in_specs, out_specs=out_specs, check_vma=False)
```

```python
import functools
import math

import jax
import jax.numpy as jnp
from jax import lax
from jax.experimental import pallas as pl
from jax.experimental.pallas import tpu as pltpu
from jax.sharding import PartitionSpec as P

SOFTEN = 0.01
CUTOFF = 3.5
F32 = jnp.float32
BF16 = jnp.bfloat16
MESH = pl.DeviceIdType.MESH


def rounded(x):
    return x.astype(BF16).astype(F32)


def split(x):
    high = x.astype(BF16)
    return high, (x - high.astype(F32)).astype(BF16)


def dot(a, b):
    return jnp.dot(a, b, preferred_element_type=F32)


def dot_t(a, b):
    return lax.dot_general(a, b, (((1,), (1,)), ((), ())), preferred_element_type=F32)


def join(parts, axis):
    return parts[0] if len(parts) == 1 else jnp.concatenate(parts, axis=axis)


def neighbours(nz, nx):
    slots = {(0, 0): 0}
    for dz in (-1, 0, 1):
        for dx in (-1, 0, 1):
            slots.setdefault((dz % nz, dx % nx), len(slots))
    return slots


def kernel(
    nz, nx, bz, bx, nb, spec, ch, lat,
    coords_hbm, species_hbm, centers_hbm, others_hbm, live_hbm, in_hbm, env_hbm, up_hbm, out_hbm,
    result_ref,
    coords_ref, species_ref, centers_ref, others_ref, live_ref, in_ref, env_ref, up_ref, out_ref,
    own, halo, tab, ct, ot, rows_live, rows_p, geo, xs, sins, coss, rad, harm,
    l2, dsilu, wts, feat, dfeat, dlat_own, env_grad, dharm, drad, gr, grad, back,
    send1, recv1, send2, recv2, load_sem,
):
    n = coords_ref.shape[-1]
    slots = neighbours(nz, nx)
    me_z, me_x = lax.axis_index("gz"), lax.axis_index("xy")
    others_list = [(key, s) for key, s in slots.items() if s > 0]

    def device(key):
        return (lax.rem(me_z + key[0], nz), lax.rem(me_x + key[1], nx))

    def mirror(key):
        return slots[((-key[0]) % nz, (-key[1]) % nx)]

    barrier = pltpu.get_barrier_semaphore()
    for key, _ in others_list:
        pl.semaphore_signal(barrier, inc=1, device_id=device(key), device_id_type=MESH)

    loads = [
        pltpu.make_async_copy(source, target, load_sem.at[k])
        for k, (source, target) in enumerate([
            (coords_hbm, coords_ref), (species_hbm, species_ref), (centers_hbm, centers_ref),
            (others_hbm, others_ref), (live_hbm, live_ref), (in_hbm, in_ref), (env_hbm, env_ref),
            (up_hbm, up_ref), (out_hbm, out_ref)])
    ]
    for load in loads:
        load.start()
    for load in loads[:5]:
        load.wait()
    lane = lax.broadcasted_iota(jnp.int32, (1, n), 1)
    for a in range(bz):
        for b in range(bx):
            alive = (lane < live_ref[a : a + 1, b : b + 1]).astype(F32)
            own[a, b] = jnp.concatenate(
                [
                    coords_ref[:, a, b, :],
                    species_ref[a, b : b + 1, :].astype(F32),
                    centers_ref[a, b : b + 1, :].astype(F32),
                    others_ref[a, b : b + 1, :].astype(F32),
                    alive,
                    jnp.zeros((1, n), F32),
                ],
                axis=0,
            )
    pl.semaphore_wait(barrier, len(others_list))
    first = []
    for key, s in others_list:
        t = mirror(key)
        copy = pltpu.make_async_remote_copy(
            src_ref=own, dst_ref=halo.at[t - 1], send_sem=send1.at[s - 1],
            recv_sem=recv1.at[t - 1], device_id=device(key), device_id_type=MESH,
        )
        copy.start()
        first.append(copy)

    for load in loads[5:]:
        load.wait()
    w_in = in_ref[...]
    w_hi = rounded(w_in)
    w_lo = w_in - w_hi
    w_rows = jnp.concatenate(
        [w_hi[:nb], w_lo[:nb], w_hi[:nb], w_hi[nb:], w_lo[nb:],
         jnp.zeros((lat - 3 * nb - 4 * spec, lat), F32)], axis=0)
    kin = (3 * nb + 4 * spec + 15) // 16 * 16
    in_t = w_rows.T.astype(BF16)[:, :kin]
    pad8 = jnp.zeros((nb, lat), F32)
    wr_hi = jnp.concatenate([w_hi[:nb], pad8], axis=0).astype(BF16)
    wr_lo = jnp.concatenate([w_lo[:nb], pad8], axis=0).astype(BF16)
    wr3 = jnp.concatenate([wr_hi, wr_hi, wr_lo], axis=1)
    env_t = env_ref[...]
    et_hi = rounded(env_t)
    et_lo = env_t - et_hi
    env_t3 = jnp.concatenate([et_hi, et_hi, et_lo], axis=1).astype(BF16)
    kpad = -(3 * ch) % lat
    env3 = jnp.concatenate(
        [et_hi, et_hi, et_lo] + ([jnp.zeros((kpad, lat), F32)] if kpad else []), axis=0
    ).T.astype(BF16)
    up = up_ref[...]
    up_hi = rounded(up)
    up_lo = up - up_hi
    up3 = jnp.concatenate([up_hi, up_hi, up_lo], axis=1).astype(BF16)
    up_t = jnp.concatenate(
        [x.T.astype(BF16) for x in (up_hi[:lat], up_hi[:lat], up_lo[:lat])]
        + [jnp.concatenate(
            [up_hi[lat:], up_hi[lat:], up_lo[lat:]]
            + ([jnp.zeros((kpad, lat), F32)] if kpad else []), axis=0).T.astype(BF16)],
        axis=1)
    out_col = jnp.broadcast_to(out_ref[...], (n, lat)).T

    cells = [(a, b) for a in range(bz - 1, 2 * bz + 1) for b in range(bx - 1, 2 * bx + 1)]
    row_n = lax.broadcasted_iota(jnp.int32, (n, n), 0)

    def hots_of(i, part):
        o = part[5:6].astype(jnp.int32)
        ct[i] = (row_n == part[4:5].astype(jnp.int32)).astype(F32).astype(BF16)
        ot[i] = (row_n == (o & 127)).astype(F32).astype(BF16)

    mine = [i for i, (a, b) in enumerate(cells) if bz <= a < 2 * bz and bx <= b < 2 * bx]
    for i in mine:
        hots_of(i, own[cells[i][0] - bz, cells[i][1] - bx])
    for copy in first:
        copy.wait()

    def place(a, b):
        return slots[((a // bz - 1) % nz, (b // bx - 1) % nx)], a % bz, b % bx

    def block(a, b):
        s, i, j = place(a, b)
        return own[i, j] if s == 0 else halo[s - 1, i, j]

    window_z = range(bz - 2, 2 * bz + 2)
    window_x = range(bx - 2, 2 * bx + 2)
    for a in window_z:
        for b in window_x:
            part = block(a, b)
            hi = rounded(part)
            tab[a, b] = jnp.concatenate([hi, part - hi], axis=0).astype(BF16)

    cx = bx + 2
    total = len(cells)
    row_s = lax.broadcasted_iota(jnp.int32, (spec, n), 0).astype(F32)
    for i, (a, b) in enumerate(cells):
        part = block(a, b)
        o = part[5:6].astype(jnp.int32)
        p = o >> 7
        if i not in mine:
            hots_of(i, part)
        hot_c, hot_o = ct[i], ot[i]
        at_c = dot(tab[a, b], hot_c)
        at_c = at_c[:8] + at_c[8:]
        around = jnp.concatenate(
            [tab[a + dz, b + dx] for dz in (-1, 0, 1) for dx in (-1, 0, 1)], axis=0)
        got = dot(around, hot_o)
        at_o = jnp.zeros((8, n), F32)
        for off in range(9):
            at_o = jnp.where(p == off, got[16 * off : 16 * off + 8] + got[16 * off + 8 : 16 * off + 16], at_o)
        diff = at_o - at_c
        up3_ = (p >= 3).astype(jnp.int32) + (p >= 6).astype(jnp.int32)
        geo[0, i : i + 1] = diff[0:1] + (up3_ - 1).astype(F32)
        geo[1, i : i + 1] = diff[1:2] + (p - 3 * up3_ - 1).astype(F32)
        geo[2, i : i + 1] = diff[2:3]
        xs[:spec, i * n : (i + 1) * n] = (row_s == at_c[3:4]).astype(F32)
        xs[spec:, i * n : (i + 1) * n] = (row_s == at_o[3:4]).astype(F32)
        rows_live[i : i + 1] = part[6:7]
        rows_p[i : i + 1] = p

    r = [geo[m] for m in range(3)]
    dist = jnp.sqrt(r[0] * r[0] + r[1] * r[1] + r[2] * r[2] + SOFTEN)
    inv = 1.0 / dist
    q = dist / CUTOFF
    rest = 1.0 - q * q
    envelope = rest * rest
    scale = inv * envelope
    s1 = jnp.sin(math.pi * q)
    c1 = jnp.cos(math.pi * q)
    s0, c0, sk, ck = jnp.zeros_like(s1), jnp.ones_like(c1), s1, c1
    for k in range(nb):
        sins[k] = sk
        coss[k] = ck
        rad[k] = sk * scale
        s0, sk = sk, 2.0 * c1 * sk - s0
        c0, ck = ck, 2.0 * c1 * ck - c0
    for m in range(3):
        harm[m] = r[m] * inv
    env_grad[...] = jnp.zeros_like(env_grad)
    geo[3] = envelope

    interior = {}
    for i, (a, b) in enumerate(cells):
        if bz <= a < 2 * bz and bx <= b < 2 * bx:
            interior[i] = (a - bz) * bx + (b - bx)

    group = 4 if total % 4 == 0 else 1
    for g in range(0, total, group):
        ids = list(range(g, g + group))
        span = slice(g * n, (g + group) * n)
        radial = join([rad[:, i, :] for i in ids], 1)
        rh = rounded(radial)
        x_s = xs[:, span]
        parts = [rh, rh, radial - rh, x_s, x_s]
        fill = kin - 3 * nb - 4 * spec
        if fill:
            parts.append(jnp.zeros((fill, group * n), F32))
        pre = dot(in_t, jnp.concatenate(parts, axis=0).astype(BF16))
        sig = 1.0 / (1.0 + jnp.exp(-pre))
        latent = pre * sig
        dsilu[:, span] = sig + latent * (1.0 - sig)
        lh, ll = split(latent)
        for t, i in enumerate(ids):
            if i in interior:
                l2[interior[i], 0] = lh[:, t * n : (t + 1) * n]
                l2[interior[i], 1] = ll[:, t * n : (t + 1) * n]
        alive = join([rows_live[i : i + 1] for i in ids], 1)
        w = dot(env_t3, jnp.concatenate([lh, ll, lh], axis=0)) * alive
        wts[:, span] = w
        msgs = jnp.concatenate(
            [w] + [w * join([harm[m, i : i + 1] for i in ids], 1) for m in range(3)], axis=0)
        mh, ml = split(msgs)
        for t, i in enumerate(ids):
            cut = slice(t * n, (t + 1) * n)
            hot_c = ct[i]
            feat[:, i * n : (i + 1) * n] = dot_t(
                jnp.concatenate([mh[:, cut], ml[:, cut]], axis=1),
                jnp.concatenate([hot_c, hot_c], axis=1)).astype(BF16)

    dfeat[...] = jnp.zeros_like(dfeat)
    row_8 = lax.broadcasted_iota(jnp.int32, (16, n), 0)
    for i, k in interior.items():
        hot_c, hot_o = ct[i], ot[i]
        p = rows_p[i : i + 1]
        env_row = geo[3, i : i + 1]
        alive = rows_live[i : i + 1]
        f_c = dot(feat[:, i * n : (i + 1) * n], hot_c)
        f_o = None
        hots = []
        for dz in range(3):
            start = i + (dz - 1) * cx - 1
            hot3 = jnp.concatenate(
                [hot_o * (p == 3 * dz + dx).astype(F32).astype(BF16) for dx in range(3)], axis=0)
            hots.append((start, hot3))
            term = dot(feat[:, start * n : (start + 3) * n], hot3)
            f_o = term if f_o is None else f_o + term
        prod4 = f_c * f_o
        prod = prod4[:ch] + prod4[ch : 2 * ch] + prod4[2 * ch : 3 * ch] + prod4[3 * ch :]
        ph, pl_ = split(prod)
        parts = [l2[k, 0], l2[k, 1], l2[k, 0], ph, pl_, ph]
        if kpad:
            parts.append(jnp.zeros((kpad, n), BF16))
        u = dot(up_t, jnp.concatenate(parts, axis=0))
        sig = 1.0 / (1.0 + jnp.exp(-u))
        hid = u * sig
        raw = jnp.sum(out_col * hid, axis=0, keepdims=True) * alive
        env_grad[i : i + 1] = raw
        e_row = raw * env_row
        e_hi = rounded(e_row)
        e_rows = jnp.where(row_8 == 0, e_hi, jnp.where(row_8 == 1, e_row - e_hi, 0.0)).astype(BF16)
        e_atom = dot_t(e_rows, hot_c)
        result_ref[3, k // bx, k % bx : k % bx + 1, :] = e_atom[0:1] + e_atom[1:2]
        d_u = out_col * (alive * env_row) * (sig + hid * (1.0 - sig))
        dh, dl = split(d_u)
        d_join = dot(up3, jnp.concatenate([dh, dl, dh], axis=0))
        dlat_own[k] = d_join[:lat]
        d_prod = jnp.concatenate([d_join[lat:]] * 4, axis=0)
        dch, dcl = split(d_prod * f_o)
        doh, dol = split(d_prod * f_c)
        dfeat[:, i * n : (i + 1) * n] += dot_t(
            jnp.concatenate([dch, dcl], axis=1), jnp.concatenate([hot_c, hot_c], axis=1))
        d_o = jnp.concatenate([doh, dol], axis=1)
        for start, hot3 in hots:
            dfeat[:, start * n : (start + 3) * n] += dot_t(
                d_o, jnp.concatenate([hot3, hot3], axis=1))

    for g in range(0, total, group):
        ids = list(range(g, g + group))
        span = slice(g * n, (g + group) * n)
        dm = []
        for i in ids:
            hot_c = ct[i]
            fh, fl = split(dfeat[:, i * n : (i + 1) * n])
            dm.append(dot(jnp.concatenate([fh, fl], axis=1), jnp.concatenate([hot_c, hot_c], axis=0)))
        dm = join(dm, 1)
        w = wts[:, span]
        dw = dm[:ch]
        for m in range(3):
            piece = dm[(m + 1) * ch : (m + 2) * ch]
            dw = dw + piece * join([harm[m, i : i + 1] for i in ids], 1)
            d_h = jnp.sum(piece * w, axis=0, keepdims=True)
            for t, i in enumerate(ids):
                dharm[m, i : i + 1] = d_h[:, t * n : (t + 1) * n]
        dw = dw * join([rows_live[i : i + 1] for i in ids], 1)
        wh, wl = split(dw)
        parts = [wh, wl, wh]
        if kpad:
            parts.append(jnp.zeros((kpad, group * n), BF16))
        d_lat = dot(env3, jnp.concatenate(parts, axis=0))
        if any(i in interior for i in ids):
            d_lat = d_lat + join(
                [dlat_own[interior[i]] if i in interior else jnp.zeros((lat, n), F32) for i in ids], 1)
        dh, dl = split(d_lat * dsilu[:, span])
        d_r = dot(wr3, jnp.concatenate([dh, dl, dh], axis=0))
        for t, i in enumerate(ids):
            drad[:, i, :] = d_r[:nb, t * n : (t + 1) * n]

    sum_s = drad[0] * sins[0]
    sum_c = drad[0] * coss[0]
    for k in range(1, nb):
        sum_s = sum_s + drad[k] * sins[k]
        sum_c = sum_c + (k + 1.0) * (drad[k] * coss[k])
    env_slope = (-4.0 / CUTOFF) * q * rest
    d_dist = (
        (math.pi / CUTOFF) * sum_c * scale
        - sum_s * scale * inv
        + (sum_s * inv + env_grad[...]) * env_slope
    )
    for m in range(3):
        d_dist = d_dist - dharm[m] * r[m] * (inv * inv)
    gr[...] = jnp.zeros_like(gr)
    for m in range(3):
        d_m = d_dist * harm[m] + dharm[m] * inv
        hi = rounded(d_m)
        gr[:, m, :] = hi
        gr[:, m + 4, :] = d_m - hi

    grad[...] = jnp.zeros_like(grad)
    second = {}

    def give(ready):
        for key, s in others_list:
            if s in second or not ready(s):
                continue
            t = mirror(key)
            second[s] = pltpu.make_async_remote_copy(
                src_ref=grad.at[s], dst_ref=back.at[t - 1], send_sem=send2.at[s - 1],
                recv_sem=recv2.at[t - 1], device_id=device(key), device_id_type=MESH,
            )
            second[s].start()

    order = sorted(range(total), key=lambda i: (-cells[i][0], cells[i][1]))
    targets = [
        {place(cells[i][0] + dz, cells[i][1] + dx)[0] for dz in (-1, 0, 1) for dx in (-1, 0, 1)}
        for i in order]
    for turn, i in enumerate(order):
        a, b = cells[i]
        g8 = gr[i]
        p = rows_p[i : i + 1]
        at_c = dot_t(jnp.concatenate([g8, jnp.zeros_like(g8)], axis=0).astype(BF16), ct[i])
        stack = [jnp.where(p == off, g8, 0.0) for off in range(9)] + [jnp.zeros_like(g8)]
        at_o = dot_t(jnp.concatenate(stack, axis=0).astype(BF16), ot[i])
        s, y, x = place(a, b)
        grad[s, y, x] -= at_c[:8]
        for off in range(9):
            s, y, x = place(a + off // 3 - 1, b + off % 3 - 1)
            grad[s, y, x] += at_o[8 * off : 8 * off + 8]
        if turn + 1 < total and b == cells[-1][1]:
            later = set().union(*targets[turn + 1 :])
            give(lambda s: s not in later)
    give(lambda s: True)
    for copy in second.values():
        copy.wait()
    for a in range(bz):
        for b in range(bx):
            acc = grad[0, a, b]
            for s in range(len(others_list)):
                acc = acc + back[s, a, b]
            acc = -(acc[:4] + acc[4:])
            result_ref[:3, a, b, :] = acc[:3]


def solution(mesh):
    nz, nx = mesh.shape["gz"], mesh.shape["xy"]

    def body(coords, species, centers, others, live_count, in_weight, env_weight, up_weight, out_weight):
        _, bz, bx, n = coords.shape
        lat, ch = env_weight.shape
        nb = 8
        spec = (in_weight.shape[0] - nb) // 2
        cells = (bz + 2) * (bx + 2)
        ns = len(neighbours(nz, nx)) - 1
        vmem = lambda shape, dtype=F32: pltpu.VMEM(shape, dtype)
        args = (coords, species, centers, others, live_count, in_weight, env_weight.T, up_weight,
                out_weight[None])
        scratch = [vmem(x.shape, x.dtype) for x in args] + [
            vmem((bz, bx, 8, n)),
            vmem((ns, bz, bx, 8, n)),
            vmem((3 * bz, 3 * bx, 16, n), BF16),
            vmem((cells, n, n), BF16),
            vmem((cells, n, n), BF16),
            vmem((cells, n)),
            vmem((cells, n), jnp.int32),
            vmem((4, cells, n)),
            vmem((2 * spec, cells * n)),
            vmem((nb, cells, n)),
            vmem((nb, cells, n)),
            vmem((nb, cells, n)),
            vmem((3, cells, n)),
            vmem((bz * bx, 2, lat, n), BF16),
            vmem((lat, cells * n)),
            vmem((ch, cells * n)),
            vmem((4 * ch, cells * n), BF16),
            vmem((4 * ch, cells * n)),
            vmem((bz * bx, lat, n)),
            vmem((cells, n)),
            vmem((3, cells, n)),
            vmem((nb, cells, n)),
            vmem((cells, 8, n)),
            vmem((ns + 1, bz, bx, 8, n)),
            vmem((ns, bz, bx, 8, n)),
        ] + [pltpu.SemaphoreType.DMA((ns,)) for _ in range(4)]
        scratch.append(pltpu.SemaphoreType.DMA((len(args),)))
        specs = [pl.BlockSpec(memory_space=pl.ANY) for _ in args]
        result = pl.pallas_call(
            functools.partial(kernel, nz, nx, bz, bx, nb, spec, ch, lat),
            out_shape=pltpu.VMEM((4, bz, bx, n), F32),
            in_specs=specs,
            out_specs=pl.BlockSpec(memory_space=pltpu.VMEM),
            scratch_shapes=scratch,
            compiler_params=pltpu.CompilerParams(collective_id=0, has_side_effects=True),
        )(*args)
        return result[3], result[:3]

    in_specs = (
        P(None, "gz", "xy", None), P("gz", "xy", None), P("gz", "xy", None), P("gz", "xy", None),
        P("gz", "xy"), P(), P(), P(), P(),
    )
    out_specs = (P("gz", "xy", None), P(None, "gz", "xy", None))
    return jax.shard_map(body, mesh=mesh, in_specs=in_specs, out_specs=out_specs, check_vma=False)
```
